512 devices in a mesh: probe: 4 (over x), seq: 128 (over y, z, core).
Axes of the slice: x: 4, y: 8, z: 8, core: 2. Of those that a mesh axis runs over, the one named last changes fastest.
Arguments:
- probe_bits: int32 [4, 128, 16384], P('probe', 'seq'), may hold values from 0 to 1
- noise_var: float32 [128, 16384], P('seq'), may hold values from 0.2 to 12
- kernel_spectrum: float32 [16384, 128], P('seq'), may hold values from 0.05 to 4, as said below
- symbol: float32 [16384, 128], P('seq'), may hold values from 0.3 to 3, as said below
- grad_prev: float32 [16384, 128], P('seq', 'probe'), may hold values from -6 to 6
Outputs:
- residual: float32 [4, 128, 16384], P('probe', 'seq')
- grad_total: float32 [16384, 128], P('seq', 'probe')
The draws below stay inside these ranges and needn't reach their ends.
Inputs may be any that keep to these rules, and one draw needn't show every extreme that they name: kernel_spectrum at frequency k equals kernel_spectrum at frequency (2097152 - k) mod 2097152. symbol at frequency k equals symbol at frequency (2097152 - k) mod 2097152.
All inputs are finite; a program needn't handle non-finite values.
Results may differ from the reference program's by a relative error of at most 0.00017.
Values sent between devices are 32-bit elements; how exact they have to be, the bound alone decides.
A program may use at most 64 MiB of HBM per device.

```python
import math
import jax
import jax.numpy as jnp
from jax import lax

COLS = 16384
ROWS = 128
SAMPLES = 2097152
PROBES = 4


def mirror(base):
    column_index = jnp.arange(COLS, dtype=jnp.int32)[:, None]
    row_index = jnp.arange(ROWS, dtype=jnp.int32)[None, :]
    frequency = column_index + COLS * row_index
    mirrored = (SAMPLES - frequency) % SAMPLES
    flipped = base[mirrored % COLS, mirrored // COLS]
    return jnp.sqrt(base * flipped)


def draw_kernel_spectrum(key, part):
    key = jax.random.fold_in(key, 11)
    base = jnp.exp(jax.random.uniform(key, (COLS, ROWS), jnp.float32, math.log(0.05), math.log(4.0)))
    return mirror(base)


def draw_symbol(key, part):
    key = jax.random.fold_in(key, 23)
    base = jnp.exp(jax.random.uniform(key, (COLS, ROWS), jnp.float32, math.log(0.3), math.log(3.0)))
    return mirror(base)


def draw_noise_var(key, part):
    key = jax.random.fold_in(key, 37)
    position = jnp.arange(ROWS, dtype=jnp.float32)[:, None] / max(ROWS - 1, 1)
    rising = 0.5 * jnp.power(12.0, position)
    rough = jnp.exp(jax.random.uniform(key, (ROWS, COLS), jnp.float32, math.log(0.7), math.log(1.4)))
    return rising * rough


def touch_ends(values, key, smallest, high):
    extent = values.shape
    place = [jax.random.randint(jax.random.fold_in(key, axis), (), 0, extent[axis]) for axis in range(len(extent))]
    values = values.at[tuple(place)].set(smallest)
    longest = extent.index(max(extent))
    place[longest] = (place[longest] + 1) % extent[longest]
    return values.at[tuple(place)].set(high)


def level_of(own_key, shape, pieces, smallest, largest):
    loudness = 1.0
    for dim, parts in pieces:
        draws = jax.random.uniform(jax.random.fold_in(jax.random.fold_in(own_key, 6), dim), (parts,), jnp.float32, smallest / len(pieces), largest / len(pieces))
        loudness = loudness * jnp.repeat(jnp.exp(draws), shape[dim] // parts).reshape((-1,) + (1,) * (len(shape) - 1 - dim))
    return loudness


def bell_draw(rng, extent, width, bound, cuts=(), held_as=jnp.bfloat16):
    result = width * jax.random.normal(rng, extent, jnp.float32)
    if cuts:
        result = result * level_of(rng, extent, cuts, -0.22, 0.18)
    return jnp.clip(result, -bound, bound).astype(held_as)


def setup_inputs(seed: int = 0) -> dict:
    key_of = jax.random.split(jax.random.key(seed), 6)
    return {
        "probe_bits": touch_ends(jax.random.randint(key_of[0], (PROBES, ROWS, COLS), 0, 2), jax.random.fold_in(key_of[0], 1), 0, 1).astype(jnp.int32),
        "noise_var": draw_noise_var(jax.random.fold_in(key_of[5], 71), 0),
        "kernel_spectrum": draw_kernel_spectrum(jax.random.fold_in(key_of[5], 71), 0),
        "symbol": draw_symbol(jax.random.fold_in(key_of[5], 71), 0),
        "grad_prev": bell_draw(key_of[4], (COLS, ROWS), 1.0, 6.0, ((0, 128), (1, 4)), jnp.float32),
    }


def to_spectrum(series):
    ordered = series.T.reshape(-1)
    spectrum = jnp.fft.fft(ordered).reshape(ROWS, COLS).T
    return jnp.real(spectrum), jnp.imag(spectrum)


def from_spectrum(real_part, imaginary):
    ordered = lax.complex(real_part, imaginary).T.reshape(-1)
    return jnp.real(jnp.fft.ifft(ordered)).reshape(COLS, ROWS).T


def reference(probe_bits, noise_var, kernel_spectrum, symbol, grad_prev):
    accumulated = jnp.zeros(grad_prev.shape, jnp.float32)
    residuals = []
    for probe_number in range(PROBES):
        sign_field = (2 * probe_bits[probe_number] - 1).astype(jnp.float32)
        base_real, base_imag = to_spectrum(sign_field)
        precond = from_spectrum(base_real / symbol, base_imag / symbol)
        again_real, again_imag = to_spectrum(precond)
        kernel_image = from_spectrum(kernel_spectrum * again_real, kernel_spectrum * again_imag) + noise_var * precond
        numerator = jnp.sum(sign_field * precond)
        curvature = jnp.sum(precond * kernel_image)
        step_size = numerator / curvature
        residual = sign_field - step_size * kernel_image
        cross_term = jnp.sum(residual * kernel_image)
        weight = -2.0 * cross_term
        resid_real, resid_imag = to_spectrum(residual)
        applied = from_spectrum(kernel_spectrum * resid_real, kernel_spectrum * resid_imag) + noise_var * residual
        adjoint = (weight / curvature) * sign_field - (2.0 * weight * step_size / curvature) * kernel_image - (2.0 * step_size) * applied
        adjoint_real, adjoint_imag = to_spectrum(adjoint)
        accumulated = accumulated - (adjoint_real * base_real + adjoint_imag * base_imag) / (SAMPLES * symbol * symbol)
        residuals.append(residual)
    return jnp.stack(residuals), grad_prev + accumulated / PROBES
```

```python
import math

import jax
import jax.numpy as jnp
import numpy as np
from jax import lax
from jax.experimental import pallas as pl
from jax.experimental.pallas import tpu as pltpu
from jax.sharding import PartitionSpec as P

MESH = pl.DeviceIdType.MESH
n = 128
f32 = jnp.float32
bf16 = jnp.bfloat16


def split_np(table):
    table = table.astype(np.float32)
    high = table.astype(jnp.bfloat16)
    low = (table - high.astype(np.float32)).astype(jnp.bfloat16)
    return high, low


def tables(samples):
    index = np.arange(n)
    product = index[:, None] * index[None, :]
    angle = 2.0 * math.pi * (product % n) / n
    cosine, sine = np.cos(angle), np.sin(angle)
    forward = np.block([[cosine, sine], [-sine, cosine]])
    inverse = np.block([[cosine, -sine], [sine, cosine]])
    turn = 2.0 * math.pi * product / (n * n)
    far = 2.0 * math.pi * product / samples
    f_high, f_low = split_np(forward)
    i_high, i_low = split_np(inverse)
    rest = [np.cos(turn), -np.sin(turn), np.cos(far), -np.sin(far)]
    return [f_high, f_low, i_high, i_low] + [part.astype(np.float32) for part in rest]


def split(x):
    high = x.astype(bf16)
    low = (x - high.astype(f32)).astype(bf16)
    return high, low


def mm(a, b):
    return jnp.dot(a, b, preferred_element_type=f32)


def table_left(t_high, t_low, data):
    high, low = split(data)
    return mm(t_high, high) + (mm(t_high, low) + mm(t_low, high))


def table_right(data, t_high, t_low):
    high, low = split(data)
    return mm(high, t_high) + (mm(low, t_high) + mm(high, t_low))


def total(x):
    return jnp.sum(jnp.sum(x, axis=0, keepdims=True), axis=1, keepdims=True)


def kernel(
    probes,
    bits_ref,
    noise_ref,
    kernel_ref,
    symbol_ref,
    prev_ref,
    fh_ref,
    fl_ref,
    ih_ref,
    il_ref,
    tc_ref,
    ts_ref,
    vc_ref,
    vs_ref,
    resid_ref,
    grad_ref,
    out1,
    in1,
    out2,
    in2,
    out3,
    in3,
    out4,
    in4,
    out5,
    in5,
    send,
    recv,
):
    me = lax.axis_index("seq")
    mine = lax.axis_index("probe")
    samples = n * n * n

    barrier = pltpu.get_barrier_semaphore()

    @pl.loop(1, n)
    def _(i):
        peer = lax.rem(me + i, n)
        pl.semaphore_signal(barrier, inc=1, device_id={"seq": peer}, device_id_type=MESH)

    for i in range(1, probes):
        other = lax.rem(mine + i, probes)
        pl.semaphore_signal(barrier, inc=1, device_id={"probe": other}, device_id_type=MESH)

    def exchange(source, target, slot):
        @pl.loop(1, n)
        def _(i):
            peer = lax.rem(me + i, n)
            pltpu.make_async_remote_copy(
                src_ref=source.at[peer],
                dst_ref=target.at[me],
                send_sem=send.at[slot],
                recv_sem=recv.at[slot],
                device_id={"seq": peer},
                device_id_type=MESH,
            ).start()

        pltpu.make_async_copy(source.at[me], target.at[me], recv.at[slot]).start()

    def arrived(target, slot):
        pltpu.make_async_copy(target, target, recv.at[slot]).wait()

    def sent(source, slot):
        part = source.at[pl.ds(0, n - 1)]
        pltpu.make_async_copy(part, part, send.at[slot]).wait()

    turn_c, turn_s = tc_ref[...], ts_ref[...]
    row_c = jnp.broadcast_to(vc_ref[pl.ds(me, 1), :], (n, n))
    row_s = jnp.broadcast_to(vs_ref[pl.ds(me, 1), :], (n, n))
    col_c = jnp.broadcast_to(tc_ref[pl.ds(me, 1), :], (n, n)).T
    col_s = jnp.broadcast_to(ts_ref[pl.ds(me, 1), :], (n, n)).T
    glob_c = col_c * row_c - col_s * row_s
    glob_s = col_c * row_s + col_s * row_c

    def forward(field):
        high, low = split(field)
        right_h, right_l = ih_ref[0:n, :], il_ref[0:n, :]
        part = mm(high, right_h) + (mm(low, right_h) + mm(high, right_l))
        real, imag = part[:, 0:n], part[:, n:]
        data = jnp.concatenate(
            [real * turn_c - imag * turn_s, real * turn_s + imag * turn_c], axis=0
        )
        full = table_left(fh_ref[...], fl_ref[...], data)
        real, imag = full[0:n], full[n:]
        return real * glob_c - imag * glob_s, real * glob_s + imag * glob_c

    def columns(real, imag):
        full = table_left(fh_ref[...], fl_ref[...], jnp.concatenate([real, imag], axis=0))
        return full[0:n], full[n:]

    sign = (2 * bits_ref[...] - 1).astype(f32).T
    noise = noise_ref[...].T
    base = forward(sign)
    out1[:, 0, :] = base[0]
    out1[:, 1, :] = base[1]
    pl.semaphore_wait(barrier, n - 1 + probes - 1)
    exchange(out1, in1, 0)
    noisy = forward(noise * sign)
    out2[:, 0, :] = noisy[0]
    out2[:, 1, :] = noisy[1]
    exchange(out2, in2, 1)
    eig = kernel_ref[...].T
    inv = 1.0 / symbol_ref[...].T

    arrived(in1, 0)
    s_real, s_imag = columns(in1[:, 0, :], in1[:, 1, :])
    scaled_real, scaled_imag = s_real * inv, s_imag * inv
    pair_real = scaled_real - eig * scaled_imag
    pair_imag = scaled_imag + eig * scaled_real
    back = table_left(ih_ref[...], il_ref[...], jnp.concatenate([pair_real, pair_imag], axis=0))
    out3[:, 0, :] = back[0:n]
    out3[:, 1, :] = back[n:]
    exchange(out3, in3, 2)
    power = s_real * s_real + s_imag * s_imag

    arrived(in3, 2)
    real, imag = in3[:, 0, :], in3[:, 1, :]
    data = jnp.concatenate(
        [real * glob_c + imag * glob_s, imag * glob_c - real * glob_s], axis=0
    )
    full = table_left(ih_ref[...], il_ref[...], data)
    real, imag = full[0:n], full[n:]
    data = jnp.concatenate(
        [real * turn_c + imag * turn_s, imag * turn_c - real * turn_s], axis=1
    )
    spatial = table_right(data, fh_ref[...], fl_ref[...]) * (1.0 / samples)
    precond, circulant = spatial[:, 0:n], spatial[:, n:]
    damped = noise * precond
    image = circulant + damped
    sums = [
        total(sign * precond),
        total(precond * image),
        total(sign * image),
        total(image * image),
    ]
    lane = lax.broadcasted_iota(jnp.int32, (1, n), 1)
    line = jnp.zeros((1, n), f32)
    for place, value in enumerate(sums):
        line = jnp.where(lane == place, value, line)
    first = forward(damped)
    second = forward(noise * image)
    for place, value in enumerate((first[0], first[1], second[0], second[1])):
        out4[:, place, 0, :] = value
    out4[:, 4, 0, :] = jnp.broadcast_to(line, (n, n))
    exchange(out4, in4, 3)

    arrived(in2, 1)
    t_real, t_imag = columns(in2[:, 0, :], in2[:, 1, :])
    t_dot = t_real * s_real + t_imag * s_imag

    arrived(in4, 3)
    lines = jnp.sum(in4[:, 4, 0, :], axis=0, keepdims=True)
    numerator, curvature, straight, squared = [
        jnp.sum(jnp.where(lane == place, lines, 0.0), axis=1, keepdims=True) for place in range(4)
    ]
    step = numerator / curvature
    weight = -2.0 * (straight - step * squared)
    over = weight / curvature
    double = 2.0 * over * step
    y_real, y_imag = columns(in4[:, 0, 0, :], in4[:, 1, 0, :])
    y_dot = y_real * s_real + y_imag * s_imag
    q_real, q_imag = columns(in4[:, 2, 0, :], in4[:, 3, 0, :])
    q_dot = q_real * s_real + q_imag * s_imag
    image_dot = eig * inv * power + y_dot
    applied_dot = eig * (power - step * image_dot) + t_dot - step * q_dot
    adjoint_dot = over * power - double * image_dot - (2.0 * step) * applied_dot
    share = adjoint_dot * (inv * inv) * (-1.0 / (samples * probes))
    width = n // probes
    for place in range(probes):
        out5[place] = share[place * width : (place + 1) * width]

    for i in range(1, probes):
        other = lax.rem(mine + i, probes)
        pltpu.make_async_remote_copy(
            src_ref=out5.at[other],
            dst_ref=in5.at[mine],
            send_sem=send.at[4],
            recv_sem=recv.at[4],
            device_id={"probe": other},
            device_id_type=MESH,
        ).start()
    pltpu.make_async_copy(out5.at[mine], in5.at[mine], recv.at[4]).start()
    resid_ref[...] = (sign - step * image).T
    sent(out1, 0)
    sent(out2, 1)
    sent(out3, 2)
    sent(out4, 3)
    arrived(in5, 4)
    own = in5[0]
    for place in range(1, probes):
        own = own + in5[place]
    grad_ref[...] = prev_ref[...] + own.T
    rest = out5.at[pl.ds(0, probes - 1)]
    pltpu.make_async_copy(rest, rest, send.at[4]).wait()


def shards(probes, probe_bits, noise_var, kernel_spectrum, symbol, grad_prev):
    width = grad_prev.shape[1]
    vmem = pl.BlockSpec(memory_space=pltpu.VMEM)
    constants = tables(n * n * n)
    pair = pltpu.VMEM((n, 2, n), f32)
    quad = pltpu.VMEM((n, 5, 1, n), f32)
    quarter = pltpu.VMEM((probes, n // probes, n), f32)
    resid, grad = pl.pallas_call(
        lambda *refs: kernel(probes, *refs),
        out_shape=(
            jax.ShapeDtypeStruct((n, n), f32),
            jax.ShapeDtypeStruct((n, width), f32),
        ),
        in_specs=[vmem] * (5 + len(constants)),
        out_specs=(vmem, vmem),
        scratch_shapes=[pair, pair, pair, pair, pair, pair, quad, quad, quarter, quarter]
        + [pltpu.SemaphoreType.DMA((5,)), pltpu.SemaphoreType.DMA((5,))],
        compiler_params=pltpu.CompilerParams(
            collective_id=0, has_side_effects=True, vmem_limit_bytes=32 * 1024 * 1024
        ),
        name="adjoint_step",
    )(
        probe_bits.reshape(n, n),
        noise_var.reshape(n, n),
        kernel_spectrum,
        symbol,
        grad_prev,
        *[jnp.asarray(part) for part in constants],
    )
    return resid.reshape(probe_bits.shape), grad


def solution(mesh):
    placed = (
        P("probe", "seq", None),
        P("seq", None),
        P("seq", None),
        P("seq", None),
        P("seq", "probe"),
    )
    probes = mesh.shape["probe"]
    return jax.shard_map(
        lambda *args: shards(probes, *args),
        mesh=mesh,
        in_specs=placed,
        out_specs=(P("probe", "seq", None), P("seq", "probe")),
        check_vma=False,
    )
```

```python
import math

import jax
import jax.numpy as jnp
import numpy as np
from jax import lax
from jax.experimental import pallas as pl
from jax.experimental.pallas import tpu as pltpu
from jax.sharding import PartitionSpec as P

MESH = pl.DeviceIdType.MESH
n = 128
f32 = jnp.float32
bf16 = jnp.bfloat16


def split_np(table):
    table = table.astype(np.float32)
    high = table.astype(jnp.bfloat16)
    low = (table - high.astype(np.float32)).astype(jnp.bfloat16)
    return high, low


def tables(samples):
    index = np.arange(n)
    product = index[:, None] * index[None, :]
    angle = 2.0 * math.pi * (product % n) / n
    cosine, sine = np.cos(angle), np.sin(angle)
    forward = np.block([[cosine, sine], [-sine, cosine]])
    inverse = np.block([[cosine, -sine], [sine, cosine]])
    turn = 2.0 * math.pi * product / (n * n)
    far = 2.0 * math.pi * product / samples
    f_high, f_low = split_np(forward)
    i_high, i_low = split_np(inverse)
    rest = [np.cos(turn), -np.sin(turn), np.cos(far), -np.sin(far)]
    dft = np.stack([i_high, i_low, f_high, f_low])
    return dft, np.stack(rest).astype(np.float32)


def split(x):
    high = x.astype(bf16)
    low = (x - high.astype(f32)).astype(bf16)
    return high, low


def mm(a, b):
    return jnp.dot(a, b, preferred_element_type=f32)


def table_left(t_high, t_low, data):
    high, low = split(data)
    return mm(t_high, high) + (mm(t_high, low) + mm(t_low, high))


def table_right(data, t_high, t_low):
    high, low = split(data)
    return mm(high, t_high) + (mm(low, t_high) + mm(high, t_low))


far_first = (4, 3, 5, 2, 6, 1, 7, 0)


def kernel(
    probes,
    bits_hbm,
    noise_hbm,
    kernel_hbm,
    symbol_hbm,
    prev_hbm,
    dft_hbm,
    turn_hbm,
    resid_ref,
    grad_ref,
    bits_ref,
    noise_ref,
    kernel_ref,
    symbol_ref,
    prev_ref,
    dft_ref,
    turn_ref,
    out1,
    in1,
    out2,
    in2,
    out3,
    in3,
    out4,
    in4,
    out5,
    in5,
    line1,
    near1,
    line2,
    near2,
    load,
    send,
    recv,
):
    me = lax.axis_index("seq")
    mine = lax.axis_index("probe")
    samples = n * n * n
    ring, plane = me // 16, lax.rem(me, 16)
    across, core = plane // 2, lax.rem(plane, 2)

    loads = [
        pltpu.make_async_copy(source, target, load.at[place])
        for place, (source, target) in enumerate(
            (
                (bits_hbm, bits_ref),
                (dft_hbm, dft_ref),
                (turn_hbm, turn_ref),
                (noise_hbm, noise_ref),
                (symbol_hbm, symbol_ref),
                (kernel_hbm, kernel_ref),
                (prev_hbm, prev_ref),
            )
        )
    ]
    for copy in loads:
        copy.start()

    inner = []
    for shift in far_first:
        spot = lax.rem(across + shift, 8) * 2
        inner += [spot + (1 - core), spot + core]

    def each_peer(act):
        @pl.loop(0, 7)
        def _(turn):
            shift = 4 + ((turn + 1) // 2) * (1 - 2 * lax.rem(turn, 2))
            start = lax.rem(ring + shift, 8) * 16
            for spot in inner:
                act(start + spot)

        for spot in inner[:-1]:
            act(ring * 16 + spot)

    barrier = pltpu.get_barrier_semaphore()

    def greet(peer):
        pl.semaphore_signal(barrier, inc=1, device_id={"seq": peer}, device_id_type=MESH)

    each_peer(greet)
    for i in range(1, probes):
        other = lax.rem(mine + i, probes)
        pl.semaphore_signal(barrier, inc=1, device_id={"probe": other}, device_id_type=MESH)

    def exchange(source, target, slot, rows):
        landing = target.at[pl.ds(me * rows, rows)]

        def put(peer):
            pltpu.make_async_remote_copy(
                src_ref=source.at[pl.ds(peer * rows, rows)],
                dst_ref=landing,
                send_sem=send.at[slot],
                recv_sem=recv.at[slot],
                device_id={"seq": peer},
                device_id_type=MESH,
            ).start()

        each_peer(put)
        own = source.at[pl.ds(me * rows, rows)]
        pltpu.make_async_copy(own, landing, recv.at[slot]).start()

    def arrived(target, slot):
        pltpu.make_async_copy(target, target, recv.at[slot]).wait()

    def sent(source, slot, rows):
        part = source.at[pl.ds(0, rows)]
        pltpu.make_async_copy(part, part, send.at[slot]).wait()

    def row(place, count):
        return pl.ds(place, n, stride=count)

    loads[0].wait()
    sign = (2 * bits_ref[...] - 1).astype(f32).T
    loads[1].wait()
    loads[2].wait()
    ih, il, fh, fl = [dft_ref.at[place] for place in range(4)]
    turn_c, turn_s = turn_ref[0], turn_ref[1]
    row_c = jnp.broadcast_to(turn_ref[2, pl.ds(me, 1), :], (n, n))
    row_s = jnp.broadcast_to(turn_ref[3, pl.ds(me, 1), :], (n, n))
    col_c = jnp.broadcast_to(turn_ref[0, pl.ds(me, 1), :], (n, n)).T
    col_s = jnp.broadcast_to(turn_ref[1, pl.ds(me, 1), :], (n, n)).T
    glob_c = col_c * row_c - col_s * row_s
    glob_s = col_c * row_s + col_s * row_c

    def forward(field, exact=False):
        right_h, right_l = ih[0:n, :], il[0:n, :]
        if exact:
            high = field.astype(bf16)
            part = mm(high, right_h) + mm(high, right_l)
        else:
            part = table_right(field, right_h, right_l)
        real, imag = part[:, 0:n], part[:, n:]
        data = jnp.concatenate(
            [real * turn_c - imag * turn_s, real * turn_s + imag * turn_c], axis=0
        )
        full = table_left(fh[...], fl[...], data)
        real, imag = full[0:n], full[n:]
        return real * glob_c - imag * glob_s, real * glob_s + imag * glob_c

    def columns(target, place, count):
        data = jnp.concatenate(
            [target[row(place, count), :], target[row(place + 1, count), :]], axis=0
        )
        full = table_left(fh[...], fl[...], data)
        return full[0:n], full[n:]

    base = forward(sign, exact=True)
    out1[row(0, 2), :] = base[0]
    out1[row(1, 2), :] = base[1]
    pl.semaphore_wait(barrier, n - 1 + probes - 1)
    exchange(out1, in1, 0, 2)
    loads[3].wait()
    noise = noise_ref[...].T
    noisy = forward(noise * sign)
    out2[row(0, 2), :] = noisy[0]
    out2[row(1, 2), :] = noisy[1]
    exchange(out2, in2, 1, 2)
    loads[4].wait()
    inv = 1.0 / symbol_ref[...].T
    loads[5].wait()
    eig = kernel_ref[...].T
    loads[6].wait()

    arrived(in1, 0)
    s_real, s_imag = columns(in1, 0, 2)
    scaled_real, scaled_imag = s_real * inv, s_imag * inv
    pair_real = scaled_real - eig * scaled_imag
    pair_imag = scaled_imag + eig * scaled_real
    back = table_left(ih[...], il[...], jnp.concatenate([pair_real, pair_imag], axis=0))
    out3[row(0, 2), :] = back[0:n]
    out3[row(1, 2), :] = back[n:]
    exchange(out3, in3, 2, 2)
    power = s_real * s_real + s_imag * s_imag
    arrived(in2, 1)
    t_real, t_imag = columns(in2, 0, 2)
    t_dot = t_real * s_real + t_imag * s_imag

    arrived(in3, 2)
    real, imag = in3[row(0, 2), :], in3[row(1, 2), :]
    data = jnp.concatenate(
        [real * glob_c + imag * glob_s, imag * glob_c - real * glob_s], axis=0
    )
    full = table_left(ih[...], il[...], data)
    real, imag = full[0:n], full[n:]
    data = jnp.concatenate(
        [real * turn_c + imag * turn_s, imag * turn_c - real * turn_s], axis=1
    )
    spatial = table_right(data, fh[...], fl[...]) * (1.0 / samples)
    precond, circulant = spatial[:, 0:n], spatial[:, n:]
    damped = noise * precond
    image = circulant + damped
    first = forward(damped)
    second = forward(noise * image)
    for place, value in enumerate(first + second):
        out4[row(place, 4), :] = value
    parts = (sign * precond, precond * image, sign * image, image * image)
    line1[...] = jnp.concatenate([jnp.sum(part, axis=0, keepdims=True) for part in parts], axis=0)

    for i in range(1, 16):
        spot = lax.rem(plane + i, 16)
        pltpu.make_async_remote_copy(
            src_ref=line1,
            dst_ref=near1.at[plane],
            send_sem=send.at[5],
            recv_sem=recv.at[5],
            device_id={"seq": ring * 16 + spot},
            device_id_type=MESH,
        ).start()
    pltpu.make_async_copy(line1, near1.at[plane], recv.at[5]).start()
    exchange(out4, in4, 3, 4)
    arrived(near1, 5)
    lines = near1[0]
    for place in range(1, 16):
        lines = lines + near1[place]
    line2[...] = lines
    for i in range(1, 8):
        spot = lax.rem(ring + i, 8)
        pltpu.make_async_remote_copy(
            src_ref=line2,
            dst_ref=near2.at[ring],
            send_sem=send.at[6],
            recv_sem=recv.at[6],
            device_id={"seq": spot * 16 + plane},
            device_id_type=MESH,
        ).start()
    pltpu.make_async_copy(line2, near2.at[ring], recv.at[6]).start()
    sent(out1, 0, 2 * (n - 1))
    sent(out2, 1, 2 * (n - 1))
    sent(out3, 2, 2 * (n - 1))
    part = near1.at[pl.ds(0, 15)]
    pltpu.make_async_copy(part, part, send.at[5]).wait()
    arrived(near2, 6)
    lines = near2[0]
    for place in range(1, 8):
        lines = lines + near2[place]
    sums = jnp.sum(lines, axis=1, keepdims=True)
    numerator, curvature, straight, squared = [sums[place : place + 1] for place in range(4)]
    step = numerator / curvature
    weight = -2.0 * (straight - step * squared)
    over = weight / curvature
    double = 2.0 * over * step
    resid_ref[...] = (sign - step * image).T
    part = near2.at[pl.ds(0, 7)]
    pltpu.make_async_copy(part, part, send.at[6]).wait()
    base_dot = over * power - (2.0 * step) * (eig * power + t_dot)
    slope = (2.0 * step * step) * eig - double
    fixed = base_dot + slope * (eig * inv * power)
    scale = (inv * inv) * (-1.0 / (samples * probes))

    arrived(in4, 3)
    y_real, y_imag = columns(in4, 0, 4)
    y_dot = y_real * s_real + y_imag * s_imag
    q_real, q_imag = columns(in4, 2, 4)
    q_dot = q_real * s_real + q_imag * s_imag
    share = (fixed + slope * y_dot + (2.0 * step * step) * q_dot) * scale
    width = n // probes
    for place in range(probes):
        out5[place] = share[place * width : (place + 1) * width]

    for i in range(1, probes):
        other = lax.rem(mine + i, probes)
        pltpu.make_async_remote_copy(
            src_ref=out5.at[other],
            dst_ref=in5.at[mine],
            send_sem=send.at[4],
            recv_sem=recv.at[4],
            device_id={"probe": other},
            device_id_type=MESH,
        ).start()
    pltpu.make_async_copy(out5.at[mine], in5.at[mine], recv.at[4]).start()
    sent(out4, 3, 4 * (n - 1))
    arrived(in5, 4)
    own = in5[0]
    for place in range(1, probes):
        own = own + in5[place]
    grad_ref[...] = prev_ref[...] + own
    rest = out5.at[pl.ds(0, probes - 1)]
    pltpu.make_async_copy(rest, rest, send.at[4]).wait()


def shards(probes, probe_bits, noise_var, kernel_spectrum, symbol, grad_prev):
    width = grad_prev.shape[1]
    vmem = pl.BlockSpec(memory_space=pltpu.VMEM)
    dft, turn = tables(n * n * n)
    block = pltpu.VMEM((n, n), f32)
    pair = pltpu.VMEM((2 * n, n), f32)
    quad = pltpu.VMEM((4 * n, n), f32)
    quarter = pltpu.VMEM((probes, width, n), f32)
    line = pltpu.VMEM((4, n), f32)
    semaphores = pltpu.SemaphoreType.DMA((7,))
    resid, grad = pl.pallas_call(
        lambda *refs: kernel(probes, *refs),
        out_shape=(
            jax.ShapeDtypeStruct((n, n), f32),
            jax.ShapeDtypeStruct((width, n), f32),
        ),
        in_specs=[pl.BlockSpec(memory_space=pl.ANY)] * 7,
        out_specs=(vmem, vmem),
        scratch_shapes=[
            pltpu.VMEM((n, n), jnp.int32),
            block,
            block,
            block,
            pltpu.VMEM((width, n), f32),
            pltpu.VMEM(dft.shape, bf16),
            pltpu.VMEM(turn.shape, f32),
        ]
        + [pair] * 6
        + [quad, quad, quarter, quarter]
        + [line, pltpu.VMEM((16, 4, n), f32), line, pltpu.VMEM((8, 4, n), f32)]
        + [semaphores] * 3,
        compiler_params=pltpu.CompilerParams(
            collective_id=0, has_side_effects=True, vmem_limit_bytes=66_000_000
        ),
        name="adjoint_step",
    )(
        probe_bits.reshape(n, n),
        noise_var.reshape(n, n),
        kernel_spectrum,
        symbol,
        grad_prev.T,
        jnp.asarray(dft),
        jnp.asarray(turn),
    )
    return resid.reshape(probe_bits.shape), grad.T


def solution(mesh):
    placed = (
        P("probe", "seq", None),
        P("seq", None),
        P("seq", None),
        P("seq", None),
        P("seq", "probe"),
    )
    probes = mesh.shape["probe"]
    return jax.shard_map(
        lambda *args: shards(probes, *args),
        mesh=mesh,
        in_specs=placed,
        out_specs=(P("probe", "seq", None), P("seq", "probe")),
        check_vma=False,
    )
```

```python
import math

import jax
import jax.numpy as jnp
import numpy as np
from jax import lax
from jax.experimental import pallas as pl
from jax.experimental.pallas import tpu as pltpu
from jax.sharding import PartitionSpec as P

MESH = pl.DeviceIdType.MESH
n = 128
f32 = jnp.float32
bf16 = jnp.bfloat16


def split_np(table):
    table = table.astype(np.float32)
    high = table.astype(jnp.bfloat16)
    low = (table - high.astype(np.float32)).astype(jnp.bfloat16)
    return high, low


def tables(samples):
    index = np.arange(n)
    product = index[:, None] * index[None, :]
    angle = 2.0 * math.pi * (product % n) / n
    cosine, sine = np.cos(angle), np.sin(angle)
    forward = np.block([[cosine, sine], [-sine, cosine]])
    inverse = np.block([[cosine, -sine], [sine, cosine]])
    turn = 2.0 * math.pi * product / (n * n)
    far = 2.0 * math.pi * product / samples
    f_high, f_low = split_np(forward)
    i_high, i_low = split_np(inverse)
    rest = [np.cos(turn), -np.sin(turn), np.cos(far), -np.sin(far)]
    dft = np.stack([i_high, i_low, f_high, f_low])
    return dft, np.stack(rest).astype(np.float32)


def split(x):
    high = x.astype(bf16)
    low = (x - high.astype(f32)).astype(bf16)
    return high, low


def mm(a, b):
    return jnp.dot(a, b, preferred_element_type=f32)


def table_left(t_high, t_low, data):
    high, low = split(data)
    return mm(
        jnp.concatenate([t_high, t_high, t_low], axis=1),
        jnp.concatenate([high, low, high], axis=0),
    )


def table_right(data, t_high, t_low):
    high, low = split(data)
    return mm(
        jnp.concatenate([high, low, high], axis=1),
        jnp.concatenate([t_high, t_high, t_low], axis=0),
    )


def far_first():
    def hops(shift):
        return min(shift, 8 - shift)

    def side(shift):
        return 0 if shift in (0, 4) else (1 if shift < 4 else -1)

    order = []
    for distance in range(8, -1, -1):
        groups = {}
        for first in range(8):
            for second in range(8):
                if hops(first) + hops(second) == distance:
                    key = (side(first), side(second))
                    groups.setdefault(key, []).append((first, second))
        keys = sorted(groups, key=lambda key: (key[0] * key[1], key))
        while any(groups.values()):
            for key in keys:
                if groups[key]:
                    order.append(groups[key].pop())
    return order


def kernel(
    probes,
    bits_hbm,
    noise_hbm,
    kernel_hbm,
    symbol_hbm,
    prev_hbm,
    dft_hbm,
    turn_hbm,
    resid_ref,
    grad_ref,
    bits_ref,
    noise_ref,
    kernel_ref,
    symbol_ref,
    prev_ref,
    dft_ref,
    turn_ref,
    out1,
    in1,
    out2,
    in2,
    out3,
    in3,
    out4,
    in4,
    out5,
    in5,
    line1,
    near1,
    line2,
    near2,
    load,
    send,
    recv,
):
    me = lax.axis_index("seq")
    mine = lax.axis_index("probe")
    samples = n * n * n
    ring, plane = me // 16, lax.rem(me, 16)
    across, core = plane // 2, lax.rem(plane, 2)

    loads = [
        pltpu.make_async_copy(source, target, load.at[place])
        for place, (source, target) in enumerate(
            (
                (bits_hbm, bits_ref),
                (dft_hbm, dft_ref),
                (turn_hbm, turn_ref),
                (noise_hbm, noise_ref),
                (symbol_hbm, symbol_ref),
                (kernel_hbm, kernel_ref),
                (prev_hbm, prev_ref),
            )
        )
    ]
    for copy in loads:
        copy.start()

    rings = [lax.rem(ring + shift, 8) * 16 for shift in range(8)]
    spots = [lax.rem(across + shift, 8) * 2 for shift in range(8)]

    def each_peer(act):
        for first, second in far_first():
            act(rings[first] + (spots[second] + (1 - core)))
            if (first, second) != (0, 0):
                act(rings[first] + (spots[second] + core))

    barrier = pltpu.get_barrier_semaphore()

    def greet(peer):
        pl.semaphore_signal(barrier, inc=1, device_id={"seq": peer}, device_id_type=MESH)

    each_peer(greet)
    for i in range(1, probes):
        other = lax.rem(mine + i, probes)
        pl.semaphore_signal(barrier, inc=1, device_id={"probe": other}, device_id_type=MESH)

    def exchange(source, target, slot, rows):
        landing = target.at[pl.ds(me * rows, rows)]

        def put(peer):
            pltpu.make_async_remote_copy(
                src_ref=source.at[pl.ds(peer * rows, rows)],
                dst_ref=landing,
                send_sem=send.at[slot],
                recv_sem=recv.at[slot],
                device_id={"seq": peer},
                device_id_type=MESH,
            ).start()

        each_peer(put)
        own = source.at[pl.ds(me * rows, rows)]
        pltpu.make_async_copy(own, landing, recv.at[slot]).start()

    def arrived(target, slot):
        pltpu.make_async_copy(target, target, recv.at[slot]).wait()

    def sent(source, slot, rows):
        part = source.at[pl.ds(0, rows)]
        pltpu.make_async_copy(part, part, send.at[slot]).wait()

    def row(place, count):
        return pl.ds(place, n, stride=count)

    loads[0].wait()
    sign = (2 * bits_ref[...] - 1).astype(f32).T
    loads[1].wait()
    loads[2].wait()
    ih, il, fh, fl = [dft_ref.at[place] for place in range(4)]
    turn_c, turn_s = turn_ref[0], turn_ref[1]
    row_c = jnp.broadcast_to(turn_ref[2, pl.ds(me, 1), :], (n, n))
    row_s = jnp.broadcast_to(turn_ref[3, pl.ds(me, 1), :], (n, n))
    col_c = jnp.broadcast_to(turn_ref[0, pl.ds(me, 1), :], (n, n)).T
    col_s = jnp.broadcast_to(turn_ref[1, pl.ds(me, 1), :], (n, n)).T
    glob_c = col_c * row_c - col_s * row_s
    glob_s = col_c * row_s + col_s * row_c

    def forward(field, exact=False):
        right_h, right_l = ih[0:n, :], il[0:n, :]
        if exact:
            high = field.astype(bf16)
            part = mm(
                jnp.concatenate([high, high], axis=1),
                jnp.concatenate([right_h, right_l], axis=0),
            )
        else:
            part = table_right(field, right_h, right_l)
        real, imag = part[:, 0:n], part[:, n:]
        data = jnp.concatenate(
            [real * turn_c - imag * turn_s, real * turn_s + imag * turn_c], axis=0
        )
        full = table_left(fh[...], fl[...], data)
        real, imag = full[0:n], full[n:]
        return real * glob_c - imag * glob_s, real * glob_s + imag * glob_c

    def columns(target, place, count):
        data = jnp.concatenate(
            [target[row(place, count), :], target[row(place + 1, count), :]], axis=0
        )
        full = table_left(fh[...], fl[...], data)
        return full[0:n], full[n:]

    base = forward(sign, exact=True)
    out1[row(0, 2), :] = base[0]
    out1[row(1, 2), :] = base[1]
    pl.semaphore_wait(barrier, n - 1 + probes - 1)
    exchange(out1, in1, 0, 2)
    loads[3].wait()
    noise = noise_ref[...].T
    noisy = forward(noise * sign)
    out2[row(0, 2), :] = noisy[0]
    out2[row(1, 2), :] = noisy[1]
    exchange(out2, in2, 1, 2)
    loads[4].wait()
    inv = 1.0 / symbol_ref[...].T
    loads[5].wait()
    eig = kernel_ref[...].T
    loads[6].wait()

    arrived(in1, 0)
    s_real, s_imag = columns(in1, 0, 2)
    scaled_real, scaled_imag = s_real * inv, s_imag * inv
    pair_real = scaled_real - eig * scaled_imag
    pair_imag = scaled_imag + eig * scaled_real
    back = table_left(ih[...], il[...], jnp.concatenate([pair_real, pair_imag], axis=0))
    out3[row(0, 2), :] = back[0:n]
    out3[row(1, 2), :] = back[n:]
    exchange(out3, in3, 2, 2)
    power = s_real * s_real + s_imag * s_imag
    arrived(in2, 1)
    t_real, t_imag = columns(in2, 0, 2)
    t_dot = t_real * s_real + t_imag * s_imag

    arrived(in3, 2)
    real, imag = in3[row(0, 2), :], in3[row(1, 2), :]
    data = jnp.concatenate(
        [real * glob_c + imag * glob_s, imag * glob_c - real * glob_s], axis=0
    )
    full = table_left(ih[...], il[...], data)
    real, imag = full[0:n], full[n:]
    data = jnp.concatenate(
        [real * turn_c + imag * turn_s, imag * turn_c - real * turn_s], axis=1
    )
    spatial = table_right(data, fh[...], fl[...]) * (1.0 / samples)
    precond, circulant = spatial[:, 0:n], spatial[:, n:]
    damped = noise * precond
    image = circulant + damped
    first = forward(damped)
    second = forward(noise * image)
    for place, value in enumerate(first + second):
        out4[row(place, 4), :] = value
    parts = (sign * precond, precond * image, sign * image, image * image)
    line1[...] = jnp.concatenate([jnp.sum(part, axis=0, keepdims=True) for part in parts], axis=0)

    for i in range(1, 16):
        spot = lax.rem(plane + i, 16)
        pltpu.make_async_remote_copy(
            src_ref=line1,
            dst_ref=near1.at[plane],
            send_sem=send.at[5],
            recv_sem=recv.at[5],
            device_id={"seq": ring * 16 + spot},
            device_id_type=MESH,
        ).start()
    pltpu.make_async_copy(line1, near1.at[plane], recv.at[5]).start()
    exchange(out4, in4, 3, 4)
    arrived(near1, 5)
    lines = near1[0]
    for place in range(1, 16):
        lines = lines + near1[place]
    line2[...] = lines
    for i in range(1, 8):
        spot = lax.rem(ring + i, 8)
        pltpu.make_async_remote_copy(
            src_ref=line2,
            dst_ref=near2.at[ring],
            send_sem=send.at[6],
            recv_sem=recv.at[6],
            device_id={"seq": spot * 16 + plane},
            device_id_type=MESH,
        ).start()
    pltpu.make_async_copy(line2, near2.at[ring], recv.at[6]).start()
    sent(out1, 0, 2 * (n - 1))
    sent(out2, 1, 2 * (n - 1))
    sent(out3, 2, 2 * (n - 1))
    part = near1.at[pl.ds(0, 15)]
    pltpu.make_async_copy(part, part, send.at[5]).wait()
    arrived(near2, 6)
    lines = near2[0]
    for place in range(1, 8):
        lines = lines + near2[place]
    sums = jnp.sum(lines, axis=1, keepdims=True)
    numerator, curvature, straight, squared = [sums[place : place + 1] for place in range(4)]
    step = numerator / curvature
    weight = -2.0 * (straight - step * squared)
    over = weight / curvature
    double = 2.0 * over * step
    resid_ref[...] = (sign - step * image).T
    part = near2.at[pl.ds(0, 7)]
    pltpu.make_async_copy(part, part, send.at[6]).wait()
    base_dot = over * power - (2.0 * step) * (eig * power + t_dot)
    slope = (2.0 * step * step) * eig - double
    fixed = base_dot + slope * (eig * inv * power)
    scale = (inv * inv) * (-1.0 / (samples * probes))

    arrived(in4, 3)
    y_real, y_imag = columns(in4, 0, 4)
    y_dot = y_real * s_real + y_imag * s_imag
    q_real, q_imag = columns(in4, 2, 4)
    q_dot = q_real * s_real + q_imag * s_imag
    share = (fixed + slope * y_dot + (2.0 * step * step) * q_dot) * scale
    width = n // probes
    for place in range(probes):
        out5[place] = share[place * width : (place + 1) * width]

    for i in sorted(range(1, probes), key=lambda i: -min(i, probes - i)):
        other = lax.rem(mine + i, probes)
        pltpu.make_async_remote_copy(
            src_ref=out5.at[other],
            dst_ref=in5.at[mine],
            send_sem=send.at[4],
            recv_sem=recv.at[4],
            device_id={"probe": other},
            device_id_type=MESH,
        ).start()
    pltpu.make_async_copy(out5.at[mine], in5.at[mine], recv.at[4]).start()
    sent(out4, 3, 4 * (n - 1))
    arrived(in5, 4)
    own = in5[0]
    for place in range(1, probes):
        own = own + in5[place]
    grad_ref[...] = prev_ref[...] + own
    rest = out5.at[pl.ds(0, probes - 1)]
    pltpu.make_async_copy(rest, rest, send.at[4]).wait()


def shards(probes, probe_bits, noise_var, kernel_spectrum, symbol, grad_prev):
    width = grad_prev.shape[1]
    vmem = pl.BlockSpec(memory_space=pltpu.VMEM)
    dft, turn = tables(n * n * n)
    block = pltpu.VMEM((n, n), f32)
    pair = pltpu.VMEM((2 * n, n), f32)
    quad = pltpu.VMEM((4 * n, n), f32)
    quarter = pltpu.VMEM((probes, width, n), f32)
    line = pltpu.VMEM((4, n), f32)
    semaphores = pltpu.SemaphoreType.DMA((7,))
    held = [
        probe_bits.reshape(n, n),
        noise_var.reshape(n, n),
        kernel_spectrum,
        symbol,
        grad_prev.T,
        jnp.asarray(dft),
        jnp.asarray(turn),
    ]
    resid, grad = pl.pallas_call(
        lambda *refs: kernel(probes, *refs),
        out_shape=(
            jax.ShapeDtypeStruct((n, n), f32),
            jax.ShapeDtypeStruct((width, n), f32),
        ),
        in_specs=[pl.BlockSpec(memory_space=pl.ANY)] * 7,
        out_specs=(vmem, vmem),
        scratch_shapes=[
            pltpu.VMEM((n, n), jnp.int32),
            block,
            block,
            block,
            pltpu.VMEM((width, n), f32),
            pltpu.VMEM(dft.shape, bf16),
            pltpu.VMEM(turn.shape, f32),
        ]
        + [pair] * 6
        + [quad, quad, quarter, quarter]
        + [line, pltpu.VMEM((16, 4, n), f32), line, pltpu.VMEM((8, 4, n), f32)]
        + [semaphores] * 3,
        compiler_params=pltpu.CompilerParams(
            collective_id=0, has_side_effects=True, vmem_limit_bytes=24_000_000
        ),
        name="adjoint_step",
    )(*[pltpu.with_memory_space_constraint(part, pltpu.MemorySpace.HBM) for part in held])
    return resid.reshape(probe_bits.shape), grad.T


def solution(mesh):
    placed = (
        P("probe", "seq", None),
        P("seq", None),
        P("seq", None),
        P("seq", None),
        P("seq", "probe"),
    )
    probes = mesh.shape["probe"]
    return jax.shard_map(
        lambda *args: shards(probes, *args),
        mesh=mesh,
        in_specs=placed,
        out_specs=(P("probe", "seq", None), P("seq", "probe")),
        check_vma=False,
    )
```

```python
import math

import jax
import jax.numpy as jnp
import numpy as np
from jax import lax
from jax.experimental import pallas as pl
from jax.experimental.pallas import tpu as pltpu
from jax.sharding import PartitionSpec as P

MESH = pl.DeviceIdType.MESH
n = 128
f32 = jnp.float32
bf16 = jnp.bfloat16


def split_np(table):
    table = table.astype(np.float32)
    high = table.astype(jnp.bfloat16)
    low = (table - high.astype(np.float32)).astype(jnp.bfloat16)
    return high, low


def tables(samples):
    index = np.arange(n)
    product = index[:, None] * index[None, :]
    angle = 2.0 * math.pi * (product % n) / n
    cosine, sine = np.cos(angle), np.sin(angle)
    forward = np.block([[cosine, sine], [-sine, cosine]])
    inverse = np.block([[cosine, -sine], [sine, cosine]])
    turn = 2.0 * math.pi * product / (n * n)
    far = 2.0 * math.pi * product / samples
    f_high, f_low = split_np(forward)
    i_high, i_low = split_np(inverse)
    rest = [np.cos(turn), -np.sin(turn), np.cos(far), -np.sin(far)]
    dft = np.stack([i_high, i_low, f_high, f_low])
    return dft, np.stack(rest).astype(np.float32)


def split(x):
    high = x.astype(bf16)
    low = (x - high.astype(f32)).astype(bf16)
    return high, low


def mm(a, b):
    return jnp.dot(a, b, preferred_element_type=f32)


def table_left(t_high, t_low, data):
    high, low = split(data)
    return mm(
        jnp.concatenate([t_high, t_high, t_low], axis=1),
        jnp.concatenate([high, low, high], axis=0),
    )


def table_right(data, t_high, t_low):
    high, low = split(data)
    return mm(
        jnp.concatenate([high, low, high], axis=1),
        jnp.concatenate([t_high, t_high, t_low], axis=0),
    )


far_first = (4, 3, 5, 2, 6, 1, 7, 0)


def kernel(
    probes,
    bits_hbm,
    noise_hbm,
    kernel_hbm,
    symbol_hbm,
    prev_hbm,
    dft_hbm,
    turn_hbm,
    resid_ref,
    grad_ref,
    bits_ref,
    noise_ref,
    kernel_ref,
    symbol_ref,
    prev_ref,
    dft_ref,
    turn_ref,
    out1,
    in1,
    out2,
    in2,
    out3,
    in3,
    out4,
    in4,
    out5,
    in5,
    line1,
    near1,
    line2,
    near2,
    load,
    send,
    recv,
):
    me = lax.axis_index("seq")
    mine = lax.axis_index("probe")
    samples = n * n * n
    ring, plane = me // 16, lax.rem(me, 16)
    across, core = plane // 2, lax.rem(plane, 2)

    loads = [
        pltpu.make_async_copy(source, target, load.at[place])
        for place, (source, target) in enumerate(
            (
                (bits_hbm, bits_ref),
                (dft_hbm, dft_ref),
                (turn_hbm, turn_ref),
                (noise_hbm, noise_ref),
                (symbol_hbm, symbol_ref),
                (kernel_hbm, kernel_ref),
                (prev_hbm, prev_ref),
            )
        )
    ]
    inner = []
    for shift in far_first:
        spot = lax.rem(across + shift, 8) * 2
        inner += [spot + (1 - core), spot + core]

    def each_peer(act):
        @pl.loop(0, 7)
        def _(turn):
            shift = 4 + ((turn + 1) // 2) * (1 - 2 * lax.rem(turn, 2))
            start = lax.rem(ring + shift, 8) * 16
            for spot in inner:
                act(start + spot)

        for spot in inner[:-1]:
            act(ring * 16 + spot)

    barrier = pltpu.get_barrier_semaphore()

    def greet(peer):
        pl.semaphore_signal(barrier, inc=1, device_id={"seq": peer}, device_id_type=MESH)

    each_peer(greet)
    for i in range(1, probes):
        other = lax.rem(mine + i, probes)
        pl.semaphore_signal(barrier, inc=1, device_id={"probe": other}, device_id_type=MESH)

    for copy in loads:
        copy.start()

    def exchange(source, target, slot, rows):
        landing = target.at[pl.ds(me * rows, rows)]

        def put(peer):
            pltpu.make_async_remote_copy(
                src_ref=source.at[pl.ds(peer * rows, rows)],
                dst_ref=landing,
                send_sem=send.at[slot],
                recv_sem=recv.at[slot],
                device_id={"seq": peer},
                device_id_type=MESH,
            ).start()

        each_peer(put)
        own = source.at[pl.ds(me * rows, rows)]
        pltpu.make_async_copy(own, landing, recv.at[slot]).start()

    def arrived(target, slot):
        pltpu.make_async_copy(target, target, recv.at[slot]).wait()

    def sent(source, slot, rows):
        part = source.at[pl.ds(0, rows)]
        pltpu.make_async_copy(part, part, send.at[slot]).wait()

    def row(place, count):
        return pl.ds(place, n, stride=count)

    loads[0].wait()
    sign = (2 * bits_ref[...] - 1).astype(f32).T
    loads[1].wait()
    loads[2].wait()
    ih, il, fh, fl = [dft_ref.at[place] for place in range(4)]
    turn_c, turn_s = turn_ref[0], turn_ref[1]
    row_c = jnp.broadcast_to(turn_ref[2, pl.ds(me, 1), :], (n, n))
    row_s = jnp.broadcast_to(turn_ref[3, pl.ds(me, 1), :], (n, n))
    col_c = jnp.broadcast_to(turn_ref[0, pl.ds(me, 1), :], (n, n)).T
    col_s = jnp.broadcast_to(turn_ref[1, pl.ds(me, 1), :], (n, n)).T
    glob_c = col_c * row_c - col_s * row_s
    glob_s = col_c * row_s + col_s * row_c

    def forward(field, exact=False):
        right_h, right_l = ih[0:n, :], il[0:n, :]
        if exact:
            high = field.astype(bf16)
            part = mm(high, right_h) + mm(high, right_l)
        else:
            part = table_right(field, right_h, right_l)
        real, imag = part[:, 0:n], part[:, n:]
        data = jnp.concatenate(
            [real * turn_c - imag * turn_s, real * turn_s + imag * turn_c], axis=0
        )
        full = table_left(fh[...], fl[...], data)
        real, imag = full[0:n], full[n:]
        return real * glob_c - imag * glob_s, real * glob_s + imag * glob_c

    def columns(target, place, count):
        data = jnp.concatenate(
            [target[row(place, count), :], target[row(place + 1, count), :]], axis=0
        )
        full = table_left(fh[...], fl[...], data)
        return full[0:n], full[n:]

    base = forward(sign, exact=True)
    out1[row(0, 2), :] = base[0]
    out1[row(1, 2), :] = base[1]
    pl.semaphore_wait(barrier, n - 1 + probes - 1)
    exchange(out1, in1, 0, 2)
    loads[3].wait()
    noise = noise_ref[...].T
    noisy = forward(noise * sign)
    out2[row(0, 2), :] = noisy[0]
    out2[row(1, 2), :] = noisy[1]
    exchange(out2, in2, 1, 2)
    loads[4].wait()
    inv = 1.0 / symbol_ref[...].T
    loads[5].wait()
    eig = kernel_ref[...].T
    loads[6].wait()

    arrived(in1, 0)
    s_real, s_imag = columns(in1, 0, 2)
    scaled_real, scaled_imag = s_real * inv, s_imag * inv
    pair_real = scaled_real - eig * scaled_imag
    pair_imag = scaled_imag + eig * scaled_real
    back = table_left(ih[...], il[...], jnp.concatenate([pair_real, pair_imag], axis=0))
    out3[row(0, 2), :] = back[0:n]
    out3[row(1, 2), :] = back[n:]
    exchange(out3, in3, 2, 2)
    power = s_real * s_real + s_imag * s_imag
    arrived(in2, 1)
    t_real, t_imag = columns(in2, 0, 2)
    t_dot = t_real * s_real + t_imag * s_imag

    arrived(in3, 2)
    real, imag = in3[row(0, 2), :], in3[row(1, 2), :]
    data = jnp.concatenate(
        [real * glob_c + imag * glob_s, imag * glob_c - real * glob_s], axis=0
    )
    full = table_left(ih[...], il[...], data)
    real, imag = full[0:n], full[n:]
    data = jnp.concatenate(
        [real * turn_c + imag * turn_s, imag * turn_c - real * turn_s], axis=1
    )
    spatial = table_right(data, fh[...], fl[...]) * (1.0 / samples)
    precond, circulant = spatial[:, 0:n], spatial[:, n:]
    damped = noise * precond
    image = circulant + damped
    first = forward(damped)
    second = forward(noise * image)
    for place, value in enumerate(first + second):
        out4[row(place, 4), :] = value
    parts = (sign * precond, precond * image, sign * image, image * image)
    line1[...] = jnp.concatenate([jnp.sum(part, axis=0, keepdims=True) for part in parts], axis=0)

    for i in range(1, 16):
        spot = lax.rem(plane + i, 16)
        pltpu.make_async_remote_copy(
            src_ref=line1,
            dst_ref=near1.at[plane],
            send_sem=send.at[5],
            recv_sem=recv.at[5],
            device_id={"seq": ring * 16 + spot},
            device_id_type=MESH,
        ).start()
    pltpu.make_async_copy(line1, near1.at[plane], recv.at[5]).start()
    exchange(out4, in4, 3, 4)
    arrived(near1, 5)
    lines = near1[0]
    for place in range(1, 16):
        lines = lines + near1[place]
    line2[...] = lines
    for i in range(1, 8):
        spot = lax.rem(ring + i, 8)
        pltpu.make_async_remote_copy(
            src_ref=line2,
            dst_ref=near2.at[ring],
            send_sem=send.at[6],
            recv_sem=recv.at[6],
            device_id={"seq": spot * 16 + plane},
            device_id_type=MESH,
        ).start()
    pltpu.make_async_copy(line2, near2.at[ring], recv.at[6]).start()
    sent(out1, 0, 2 * (n - 1))
    sent(out2, 1, 2 * (n - 1))
    sent(out3, 2, 2 * (n - 1))
    part = near1.at[pl.ds(0, 15)]
    pltpu.make_async_copy(part, part, send.at[5]).wait()
    arrived(near2, 6)
    lines = near2[0]
    for place in range(1, 8):
        lines = lines + near2[place]
    sums = jnp.sum(lines, axis=1, keepdims=True)
    numerator, curvature, straight, squared = [sums[place : place + 1] for place in range(4)]
    step = numerator / curvature
    weight = -2.0 * (straight - step * squared)
    over = weight / curvature
    double = 2.0 * over * step
    resid_ref[...] = (sign - step * image).T
    part = near2.at[pl.ds(0, 7)]
    pltpu.make_async_copy(part, part, send.at[6]).wait()
    base_dot = over * power - (2.0 * step) * (eig * power + t_dot)
    slope = (2.0 * step * step) * eig - double
    fixed = base_dot + slope * (eig * inv * power)
    scale = (inv * inv) * (-1.0 / (samples * probes))

    arrived(in4, 3)
    y_real, y_imag = columns(in4, 0, 4)
    y_dot = y_real * s_real + y_imag * s_imag
    q_real, q_imag = columns(in4, 2, 4)
    q_dot = q_real * s_real + q_imag * s_imag
    share = (fixed + slope * y_dot + (2.0 * step * step) * q_dot) * scale
    width = n // probes
    for place in range(probes):
        out5[place] = share[place * width : (place + 1) * width]

    for i in sorted(range(1, probes), key=lambda i: -min(i, probes - i)):
        other = lax.rem(mine + i, probes)
        pltpu.make_async_remote_copy(
            src_ref=out5.at[other],
            dst_ref=in5.at[mine],
            send_sem=send.at[4],
            recv_sem=recv.at[4],
            device_id={"probe": other},
            device_id_type=MESH,
        ).start()
    pltpu.make_async_copy(out5.at[mine], in5.at[mine], recv.at[4]).start()
    sent(out4, 3, 4 * (n - 1))
    arrived(in5, 4)
    own = in5[0]
    for place in range(1, probes):
        own = own + in5[place]
    grad_ref[...] = prev_ref[...] + own
    rest = out5.at[pl.ds(0, probes - 1)]
    pltpu.make_async_copy(rest, rest, send.at[4]).wait()


def shards(probes, probe_bits, noise_var, kernel_spectrum, symbol, grad_prev):
    width = grad_prev.shape[1]
    vmem = pl.BlockSpec(memory_space=pltpu.VMEM)
    dft, turn = tables(n * n * n)
    block = pltpu.VMEM((n, n), f32)
    pair = pltpu.VMEM((2 * n, n), f32)
    quad = pltpu.VMEM((4 * n, n), f32)
    quarter = pltpu.VMEM((probes, width, n), f32)
    line = pltpu.VMEM((4, n), f32)
    semaphores = pltpu.SemaphoreType.DMA((7,))
    held = [
        probe_bits.reshape(n, n),
        noise_var.reshape(n, n),
        kernel_spectrum,
        symbol,
        grad_prev.T,
        jnp.asarray(dft),
        jnp.asarray(turn),
    ]
    resid, grad = pl.pallas_call(
        lambda *refs: kernel(probes, *refs),
        out_shape=(
            jax.ShapeDtypeStruct((n, n), f32),
            jax.ShapeDtypeStruct((width, n), f32),
        ),
        in_specs=[pl.BlockSpec(memory_space=pl.ANY)] * 7,
        out_specs=(vmem, vmem),
        scratch_shapes=[
            pltpu.VMEM((n, n), jnp.int32),
            block,
            block,
            block,
            pltpu.VMEM((width, n), f32),
            pltpu.VMEM(dft.shape, bf16),
            pltpu.VMEM(turn.shape, f32),
        ]
        + [pair] * 6
        + [quad, quad, quarter, quarter]
        + [line, pltpu.VMEM((16, 4, n), f32), line, pltpu.VMEM((8, 4, n), f32)]
        + [semaphores] * 3,
        compiler_params=pltpu.CompilerParams(
            collective_id=0, has_side_effects=True, vmem_limit_bytes=24_000_000
        ),
        name="adjoint_step",
    )(*[pltpu.with_memory_space_constraint(part, pltpu.MemorySpace.HBM) for part in held])
    return resid.reshape(probe_bits.shape), grad.T


def solution(mesh):
    placed = (
        P("probe", "seq", None),
        P("seq", None),
        P("seq", None),
        P("seq", None),
        P("seq", "probe"),
    )
    probes = mesh.shape["probe"]
    return jax.shard_map(
        lambda *args: shards(probes, *args),
        mesh=mesh,
        in_specs=placed,
        out_specs=(P("probe", "seq", None), P("seq", "probe")),
        check_vma=False,
    )
```
